32 devices in a mesh: paths: 8 (over z, core), stocks: 4 (over y, x).
Axes of the slice: x: 2, y: 2, z: 4, core: 2. Of those that a mesh axis runs over, the one named last changes fastest.
Arguments:
- prices: bfloat16 [256, 131072], P('stocks', 'paths'), may hold values from -18 to 18
- loadings: bfloat16 [256, 32], P('stocks'), may hold values from -0.25 to 0.25
- basis_w: float32 [32, 512], replicated, may hold values from -1 to 1
- basis_bias: float32 [512], replicated, may hold values from -1 to 1
- payoff: bfloat16 [131072], P('paths'), may hold values from -4 to 4
- in_fit: int32 [131072], P('paths'), may hold values 0 or 1
- cotangent: bfloat16 [256, 131072], P('stocks', 'paths'), may hold values from -6 to 6
- shocks: bfloat16 [4, 256, 131072], P(None, 'stocks', 'paths'), may hold values from -6 to 6
- corr_gen: bfloat16 [256, 256], replicated, may hold values from -0.375 to 0.375
- basket: float32 [256], replicated, may hold values from 0.2 to 2
- exercise: int32 [4, 131072], P(None, 'paths'), may hold values 0 or 1
- bucket: int32 [4, 131072], P(None, 'paths'), may hold values from 0 to 255
Outputs:
- delta_out: float32 [256, 131072], P('stocks', 'paths')
- surface: float32 [256, 256], P('stocks', 'paths')
The draws below stay inside these ranges and needn't reach their ends.
All inputs are finite; a program needn't handle non-finite values. No bound on the sum of `in_fit` or of `exercise` on one device may be relied on, other than what follows from the above.
Results may differ from the reference program's by a relative error of at most 0.003.
Values may be sent and summed in bfloat16 or wider, within the bound.
A program may use at most 192 MiB of HBM per device.

```python
import jax
import jax.numpy as jnp
from jax import lax

S = 256
K = 32
B = 512
NK = 256
STEPS = 4
PATHS = 131072


def price_state(key):
    price_key = jax.random.fold_in(key, 101)
    position = jnp.arange(PATHS, dtype=jnp.float32) / PATHS
    random_part = jax.random.truncated_normal(price_key, -6.0, 6.0, (S, PATHS), jnp.float32)
    path_scale = jnp.exp(jnp.log(3.0) * position)
    return (random_part * path_scale[None, :]).astype(jnp.bfloat16)


def loading_table(key):
    load_key = jax.random.fold_in(key, 102)
    limit = min(4.0, 0.25 * S ** 0.5)
    values = jax.random.truncated_normal(load_key, -limit, limit, (S, K), jnp.float32) / S ** 0.5
    values = jnp.clip(values, -0.25, 0.25)
    return values.astype(jnp.bfloat16)


def draw_prices(key, part):
    return price_state(key)


def draw_loadings(key, part):
    return loading_table(key)


def draw_payoff(key, part):
    prices = price_state(key)
    loads = loading_table(key)
    factors = lax.dot_general(loads, prices, (((0,), (0,)), ((), ())), preferred_element_type=jnp.float32)
    directions = jax.random.normal(jax.random.fold_in(key, 103), (2, K), jnp.float32) / K ** 0.5
    levels = jnp.dot(directions, factors, preferred_element_type=jnp.float32, precision=lax.Precision.HIGHEST)
    shaped = 2.0 * jnp.tanh(0.7 * levels[0]) + 0.8 * jnp.abs(jnp.tanh(levels[1])) - 0.4
    noise = 0.3 * jax.random.truncated_normal(jax.random.fold_in(key, 104), -3.0, 3.0, (PATHS,), jnp.float32)
    return jnp.clip(shaped + noise, -4.0, 4.0).astype(jnp.bfloat16)


def with_ends(result, key, low, high):
    longest = result.shape.index(max(result.shape))
    spots = []
    for shift in (0, 1):
        where = [jax.random.randint(jax.random.fold_in(key, axis), (), 0, length) for axis, length in enumerate(result.shape)]
        where[longest] = (where[longest] + shift) % result.shape[longest]
        spots.append(tuple(where))
    return result.at[spots[0]].set(low).at[spots[1]].set(high)


def level_of(own_key, dims, shards, least, top_value):
    level = 1.0
    for axis_at, blocks in shards:
        draws = jax.random.uniform(jax.random.fold_in(jax.random.fold_in(own_key, 6), axis_at), (blocks,), jnp.float32, least / len(shards), top_value / len(shards))
        level = level * jnp.repeat(jnp.exp(draws), dims[axis_at] // blocks).reshape((-1,) + (1,) * (len(dims) - 1 - axis_at))
    return level


def scatter_about(key, dims, scale, bound, shards=(), kind=jnp.bfloat16):
    result = scale * jax.random.normal(key, dims, jnp.float32)
    if shards:
        result = result * level_of(key, dims, shards, -0.22, 0.18)
    return jnp.clip(result, -bound, bound).astype(kind)


def setup_inputs(seed: int = 0) -> dict:
    streams_of = jax.random.split(jax.random.key(seed), 13)
    return {
        "prices": draw_prices(jax.random.fold_in(streams_of[12], 71), 0),
        "loadings": draw_loadings(jax.random.fold_in(streams_of[12], 71), 0),
        "basis_w": scatter_about(streams_of[2], (K, B), K ** -0.5, 1.0, (), jnp.float32),
        "basis_bias": jnp.clip(jax.random.uniform(streams_of[3], (B,), jnp.float32, -1.0, 1.0), -1.0, 1.0),
        "payoff": draw_payoff(jax.random.fold_in(streams_of[12], 71), 0),
        "in_fit": with_ends((jax.random.randint(streams_of[5], (PATHS,), 0, 3) < 2).astype(jnp.int32), jax.random.fold_in(streams_of[5], 1), 0, 1),
        "cotangent": scatter_about(streams_of[6], (S, PATHS), 1.0, 6.0, ((0, 4), (1, 8))),
        "shocks": scatter_about(streams_of[7], (STEPS, S, PATHS), 1.0, 6.0, ((1, 4), (2, 8))),
        "corr_gen": scatter_about(streams_of[8], (S, S), S ** -0.5, 0.375),
        "basket": jnp.clip(jax.random.uniform(streams_of[9], (S,), jnp.float32, 0.2, 2.0), 0.2, 2.0),
        "exercise": with_ends((jax.random.randint(streams_of[10], (STEPS, PATHS), 0, 4) < 1).astype(jnp.int32), jax.random.fold_in(streams_of[10], 1), 0, 1),
        "bucket": with_ends(jax.random.randint(streams_of[11], (STEPS, PATHS), 0, NK), jax.random.fold_in(streams_of[11], 1), 0, NK - 1).astype(jnp.int32),
    }


time_step = 0.25
ridge_weight = 0.1

def make_basis(factors, basis_w, basis_bias):
    raised = jnp.dot(basis_w.T.astype(jnp.float32), factors.astype(jnp.float32), preferred_element_type=jnp.float32, precision=lax.Precision.HIGHEST) + basis_bias[:, None]
    return jnp.tanh(raised).astype(jnp.bfloat16)

def regression_sums(basis, payoff, in_fit):
    picked = basis * in_fit.astype(jnp.bfloat16)[None, :]
    gram_sums = lax.dot_general(picked.astype(jnp.float32), basis.astype(jnp.float32), (((1,), (1,)), ((), ())), preferred_element_type=jnp.float32)
    moment = jnp.dot(picked.astype(jnp.float32), payoff.astype(jnp.float32), preferred_element_type=jnp.float32)
    return (gram_sums, moment)

def solve_coefficients(gram_sums, moment, path_count):
    system = gram_sums / path_count + ridge_weight * jnp.eye(gram_sums.shape[0], dtype=jnp.float32)
    cholesky_factor = jnp.linalg.cholesky(system)
    return jax.scipy.linalg.cho_solve((cholesky_factor, True), moment / path_count)

def reference(prices, loadings, basis_w, basis_bias, payoff, in_fit, cotangent, shocks, corr_gen, basket, exercise, bucket):
    factors = lax.dot_general(loadings.astype(jnp.float32), prices.astype(jnp.float32), (((0,), (0,)), ((), ())), preferred_element_type=jnp.float32)
    basis = make_basis(factors, basis_w, basis_bias)
    gram_sums, moment = regression_sums(basis, payoff, in_fit)
    coefficients = solve_coefficients(gram_sums, moment, PATHS * 1.0)
    continuation = jnp.dot(coefficients.astype(jnp.float32), basis.astype(jnp.float32), preferred_element_type=jnp.float32, precision=lax.Precision.HIGHEST)
    adjoint = cotangent.astype(jnp.float32)
    surface = jnp.zeros((S, NK), jnp.float32)
    strikes = jnp.arange(NK, dtype=jnp.int32)
    for date_index in range(STEPS - 1, -1, -1):
        mixed_rows = jnp.dot(corr_gen.astype(jnp.float32), adjoint.astype(jnp.bfloat16).astype(jnp.float32), preferred_element_type=jnp.float32)
        adjoint = adjoint + time_step * mixed_rows + exercise[date_index].astype(jnp.float32)[None, :] * continuation[None, :] * basket[:, None]
        vega_terms = (adjoint * shocks[date_index].astype(jnp.float32)).astype(jnp.bfloat16)
        one_hot = (bucket[date_index][:, None] == strikes[None, :]).astype(jnp.bfloat16)
        surface = surface + jnp.dot(vega_terms.astype(jnp.float32), one_hot.astype(jnp.float32), preferred_element_type=jnp.float32)
    return (adjoint, surface)
```

```python
import functools

import jax
import jax.numpy as jnp
from jax import lax
from jax.experimental import pallas as pl
from jax.experimental.pallas import tpu as pltpu
from jax.sharding import PartitionSpec as P

NK = 256
STEPS = 4
SUB = 8
BLOCK = 128
PACK = 16
TILE = 1024
LAG = 3

time_step = 0.25
ridge_weight = 0.1
HIGHEST = lax.Precision.HIGHEST
MESH = pl.DeviceIdType.MESH
F32 = jnp.float32
BF16 = jnp.bfloat16
LANES = (((1,), (1,)), ((), ()))


def pieces(value):
    high = value.astype(BF16)
    rest = value - high.astype(F32)
    middle = rest.astype(BF16)
    low = (rest - middle.astype(F32)).astype(BF16)
    return high, middle, low


def sweep_block(tile_ref):
    size = tile_ref.shape[0]
    rows = lax.broadcasted_iota(jnp.int32, (SUB, size), 0)
    lanes = lax.broadcasted_iota(jnp.int32, (SUB, size), 1)
    all_lanes = lax.broadcasted_iota(jnp.int32, (size, size), 1)
    for start in range(0, size, SUB):
        whole = tile_ref[...]
        columns = [
            jnp.broadcast_to(whole[:, start + c : start + c + 1], (size, size)) for c in range(SUB)
        ]
        pivots = [columns[c][start : start + SUB] for c in range(SUB)]
        strip = whole[start : start + SUB]
        inside = (lanes >= start) & (lanes < start + SUB)
        strip = jnp.where(inside, jnp.where(lanes - start == rows, 1.0, 0.0), strip)
        for j in range(SUB):
            inverse = 1.0 / pivots[j][j : j + 1]
            chosen = strip[j : j + 1] * inverse
            strip = jnp.where(rows == j, chosen, strip - pivots[j] * chosen)
            for c in range(j + 1, SUB):
                moved = pivots[c][j : j + 1] * inverse
                pivots[c] = jnp.where(rows == j, moved, pivots[c] - pivots[j] * moved)
        inside_all = (all_lanes >= start) & (all_lanes < start + SUB)
        updated = jnp.where(inside_all, 0.0, whole)
        for c in range(SUB):
            updated = updated - columns[c] * strip[c : c + 1]
        tile_ref[...] = updated
        tile_ref[start : start + SUB, :] = strip


def solve(system_ref, moment_ref, inverse_ref, reduced_ref, tile_ref, out_ref, each):
    size = system_ref.shape[0]
    strip_lanes = lax.broadcasted_iota(jnp.int32, (BLOCK, size), 1)

    def eliminate(k, carry):
        here = pl.ds(pl.multiple_of(k * BLOCK, BLOCK), BLOCK)
        each(k)
        tile_ref[...] = system_ref[here, here]
        sweep_block(tile_ref)
        inverse = tile_ref[...]
        inverse_ref[here, :] = inverse
        right = jnp.where(strip_lanes >= (k + 1) * BLOCK, system_ref[here, :], 0.0)
        reduced = jnp.dot(inverse, right, preferred_element_type=jnp.float32, precision=HIGHEST)
        reduced_ref[here, :] = reduced
        system_ref[...] -= jnp.dot(
            system_ref[:, here], reduced, preferred_element_type=jnp.float32, precision=HIGHEST
        )
        moment_ref[...] -= jnp.dot(
            moment_ref[:, here], reduced, preferred_element_type=jnp.float32, precision=HIGHEST
        )
        return carry

    blocks = size // BLOCK
    lax.fori_loop(0, blocks, eliminate, 0)
    out_ref[...] = jnp.zeros_like(out_ref)

    def substitute(step, carry):
        k = blocks - 1 - step
        here = pl.ds(pl.multiple_of(k * BLOCK, BLOCK), BLOCK)
        known = lax.dot_general(
            out_ref[...],
            reduced_ref[here, :],
            LANES,
            preferred_element_type=jnp.float32,
            precision=HIGHEST,
        )
        out_ref[:, here] = (
            jnp.dot(
                moment_ref[:, here],
                inverse_ref[here, :],
                preferred_element_type=jnp.float32,
                precision=HIGHEST,
            )
            - known
        )
        return carry

    lax.fori_loop(0, blocks, substitute, 0)


def block_pairs(functions):
    count = functions // BLOCK
    return [(i, j) for i in range(count) for j in range(i + 1)]


def sum_rows(functions, path_devices):
    rows = len(block_pairs(functions)) * BLOCK + functions // BLOCK
    unit = SUB * path_devices
    return -(-rows // unit) * unit


def step_kernel(
    n_p, n_s, path_count,
    prices_ref, loadings_ref, basis_w_ref, bias_ref, payoff_ref, fit_ref, cot_ref, shocks_ref,
    corr_ref, basket_ref, exercise_ref, bucket_ref,
    delta_ref, surface_ref,
    prices_v, whole, shocks_v, delta_v, factor_send, factor_recv, weights_v, basis_v,
    acc, core_recv, z_recv, piece, x_recv, total,
    system, moment, inverse, reduced, tile_v, coef, value_v, split_v, basket_v, surface_acc, surface_recv,
    local_sem, delta_sem, f_send, f_recv, ag_send, ag_recv, c1_send, c1_recv, z_send, z_rcv,
    x_send, x_rcv, z4_send, z4_recv, c5_send, c5_recv, v_send, v_recv, s_send, s_recv,
):
    p = lax.axis_index("paths")
    s = lax.axis_index("stocks")
    core = lax.rem(p, 2)
    z = p // 2
    n_z = n_p // 2
    rows, paths = cot_ref.shape
    rank, functions = basis_w_ref.shape
    share = paths // n_s
    tile = min(TILE, share)
    chunks = paths // tile
    share_tiles = share // tile
    square = n_s == 4

    def stock(r):
        return (p, lax.bitwise_xor(s, r))

    def columns(i):
        return pl.ds(pl.multiple_of(i * tile, tile), tile)

    def remote(source, target, send, recv, device):
        return pltpu.make_async_remote_copy(
            src_ref=source, dst_ref=target, send_sem=send, recv_sem=recv,
            device_id=device, device_id_type=MESH,
        )

    prices_copy = pltpu.make_async_copy(prices_ref, prices_v, local_sem.at[0])
    prices_copy.start()
    own_copy = pltpu.make_async_copy(cot_ref, whole.at[s], local_sem.at[1])
    own_copy.start()
    shocks_copy = pltpu.make_async_copy(shocks_ref, shocks_v, local_sem.at[2])
    shocks_copy.start()

    barrier = pltpu.get_barrier_semaphore()
    for r in range(1, n_s):
        pl.semaphore_signal(barrier, inc=1, device_id=stock(r), device_id_type=MESH)
    for d in range(1, n_p):
        pl.semaphore_signal(
            barrier, inc=1, device_id=(lax.rem(p + d, n_p), s), device_id_type=MESH
        )

    def factor_copy(r):
        return remote(
            factor_send.at[r], factor_recv.at[r], f_send.at[r], f_recv.at[r], stock(r)
        )

    prices_copy.wait()
    for r in list(range(1, n_s)) + [0]:
        owner = lax.bitwise_xor(s, r)

        def partial(t, carry, r=r, owner=owner):
            here = pl.ds(pl.multiple_of(owner * share + t * tile, tile), tile)
            factor_send[r, :, columns(t)] = lax.dot_general(
                loadings_ref[...], prices_v[:, here], (((0,), (0,)), ((), ())),
                preferred_element_type=F32,
            )
            return carry

        lax.fori_loop(0, share_tiles, partial, 0)
        if r == 1:
            pl.semaphore_wait(barrier, n_s + n_p - 2)
        if r > 0:
            factor_copy(r).start()

    half = rows // 2

    def own_chunk(kind, r, k):
        return remote(
            cot_ref.at[:, columns(k)], whole.at[s, :, columns(k)],
            ag_send.at[kind, k], ag_recv.at[kind, k], stock(r),
        )

    def passed_chunk(kind, source, target, k):
        block = lax.bitwise_xor(s, source)
        part = pl.ds((source - 1) * half, half)
        return remote(
            whole.at[block, part, columns(k)], whole.at[block, part, columns(k)],
            ag_send.at[kind, k], ag_recv.at[kind, k], stock(target),
        )

    def chunk_copies(k):
        if square:
            return [
                own_chunk(0, 1, k), own_chunk(1, 2, k),
                passed_chunk(2, 1, 2, k), passed_chunk(3, 2, 1, k),
            ]
        return [own_chunk(r - 1, r, k) for r in range(1, n_s)]

    def guarded(condition, action):
        if isinstance(condition, bool):
            if condition:
                action()
        else:
            pl.when(condition)(action)

    def gather_slot(k):
        def send():
            if square:
                own_chunk(0, 1, k).start()
                own_chunk(1, 2, k).start()
            else:
                for r in range(1, n_s):
                    own_chunk(r - 1, r, k).start()

        def forward():
            j = k - LAG
            own_chunk(0, 1, j).wait_recv()
            passed_chunk(2, 1, 2, j).start()
            own_chunk(1, 2, j).wait_recv()
            passed_chunk(3, 2, 1, j).start()

        guarded(k < chunks, send)
        if square:
            if isinstance(k, int):
                guarded(k >= LAG and k - LAG < chunks, forward)
            else:
                guarded(jnp.logical_and(k >= LAG, k - LAG < chunks), forward)

    gather_slot(0)
    gather_slot(1)

    weight_parts = pieces(basis_w_ref[...])
    bias_parts = pieces(bias_ref[...])
    packed = [weight_parts[i] for i in (0, 0, 1, 0, 1, 2)]
    spare = jnp.zeros((PACK - 3, functions), F32)
    tail = jnp.concatenate([part.astype(F32) for part in bias_parts] + [spare], axis=0)
    stacked = jnp.concatenate([part.astype(F32) for part in packed] + [tail], axis=0)
    weights_v[...] = stacked.T.astype(BF16)
    acc[...] = jnp.zeros_like(acc)
    surface_acc[...] = jnp.zeros_like(surface_acc)

    step = time_step * corr_ref[...].astype(F32)
    own_rows = pl.ds(pl.multiple_of(s * rows, rows), rows)
    own_step = time_step * corr_ref[own_rows, :].astype(F32)
    own_basket = jnp.sum(
        jnp.where(
            lax.broadcasted_iota(jnp.int32, own_step.shape, 1)
            == lax.broadcasted_iota(jnp.int32, own_step.shape, 0) + s * rows,
            basket_ref[...], 0.0,
        ), axis=1, keepdims=True,
    )
    identity = jnp.where(
        lax.broadcasted_iota(jnp.int32, own_step.shape, 1)
        == lax.broadcasted_iota(jnp.int32, own_step.shape, 0) + s * rows, 1.0, 0.0,
    )
    power = own_step
    for k in range(STEPS):
        if k > 0:
            basket_v[k] = jnp.broadcast_to(
                own_basket + jnp.sum(power * basket_ref[...], axis=1, keepdims=True),
                basket_v.shape[1:],
            )
            power = power + own_step + jnp.dot(
                power, step, preferred_element_type=F32, precision=HIGHEST
            )
        else:
            basket_v[k] = jnp.broadcast_to(own_basket, basket_v.shape[1:])
        high, middle, _ = pieces(power + identity)
        split_v[k * rows : (k + 1) * rows, 0 : n_s * rows] = high
        split_v[k * rows : (k + 1) * rows, n_s * rows :] = middle

    for r in range(1, n_s):
        factor_copy(r).wait_recv()
    pairs = block_pairs(functions)
    span = functions // BLOCK
    moment_at = len(pairs) * BLOCK
    share_start = s * share
    wide = 2 * BLOCK

    def basis_tile(t, carry):
        here = columns(t)
        factors = factor_send[0, :, here]
        for r in range(1, n_s):
            factors = factors + factor_recv[r, :, here]
        high, middle, low = pieces(factors)
        ones = jnp.where(
            lax.broadcasted_iota(jnp.int32, (PACK, tile), 0) < 3, 1.0, 0.0
        ).astype(BF16)
        packed_factors = jnp.concatenate([high, middle, high, low, middle, high, ones], axis=0)
        raised = jnp.dot(weights_v[...], packed_factors, preferred_element_type=F32)
        basis = jnp.tanh(raised).astype(BF16)
        basis_v[:, here] = basis
        from_start = pl.ds(pl.multiple_of(share_start + t * tile, tile), tile)
        picked = basis * fit_ref[:, from_start].astype(BF16)
        for i in range(0, span, 2):
            count = min(2, span - i)
            for j in range(0, i + 1, 2):
                part = lax.dot_general(
                    basis[i * BLOCK : (i + count) * BLOCK],
                    picked[j * BLOCK : min(j + 2, span) * BLOCK],
                    LANES, preferred_element_type=F32,
                )
                for a in range(count):
                    for b in range(min(2, span - j)):
                        if (i + a, j + b) in pairs:
                            at = pairs.index((i + a, j + b)) * BLOCK
                            acc[at : at + BLOCK, :] += part[
                                a * BLOCK : (a + 1) * BLOCK, b * BLOCK : (b + 1) * BLOCK
                            ]
        cash = jnp.broadcast_to(payoff_ref[:, from_start], (2 * SUB, tile))
        cash_sum = lax.dot_general(cash, picked, LANES, preferred_element_type=F32)
        for i in range(span):
            acc[moment_at + i : moment_at + i + 1, :] += cash_sum[
                0:1, i * BLOCK : (i + 1) * BLOCK
            ]
        return carry

    lax.fori_loop(0, share_tiles, basis_tile, 0)
    gather_slot(2)

    half_rows = acc.shape[0] // 2
    piece_rows = acc.shape[0] // n_p
    partner = (p + 1 - 2 * core, s)

    def half_at(c):
        return pl.ds(pl.multiple_of(c * half_rows, SUB), half_rows)

    def piece_at(c, zz):
        return pl.ds(pl.multiple_of(c * half_rows + zz * piece_rows, SUB), piece_rows)

    def z_peer(d):
        other = lax.rem(z + d, n_z)
        return other, (2 * other + core, s)

    core_copy = remote(
        acc.at[half_at(1 - core)], core_recv, c1_send.at[0], c1_recv.at[0], partner
    )
    core_copy.start()
    core_copy.wait_recv()
    acc[half_at(core), :] += core_recv[...]
    z_copies = []
    for d in range(1, n_z):
        other, device = z_peer(d)
        z_copies.append(
            remote(acc.at[piece_at(core, other)], z_recv.at[d], z_send.at[d], z_rcv.at[d], device)
        )
    for copy in z_copies:
        copy.start()
    for copy in z_copies:
        copy.wait_recv()
    mine = acc[piece_at(core, z), :]
    for d in range(1, n_z):
        mine = mine + z_recv[d]
    piece[...] = mine
    x_copies = [
        remote(piece, x_recv.at[r], x_send.at[r], x_rcv.at[r], stock(r)) for r in range(1, n_s)
    ]
    for copy in x_copies:
        copy.start()
    gather_slot(3)
    gather_slot(4)
    for copy in x_copies:
        copy.wait_recv()
    mine = piece[...]
    for r in range(1, n_s):
        mine = mine + x_recv[r]
    total[piece_at(core, z), :] = mine

    def spread(slot, zz):
        return remote(
            total.at[piece_at(core, zz)], total.at[piece_at(core, zz)],
            c5_send.at[slot], c5_recv.at[slot], partner,
        )

    back_copies = []
    for d in range(1, n_z):
        _, device = z_peer(d)
        back_copies.append(
            remote(
                total.at[piece_at(core, z)], total.at[piece_at(core, z)],
                z4_send.at[d], z4_recv.at[d], device,
            )
        )
    for copy in back_copies:
        copy.start()
    core_copies = [spread(0, z)]
    core_copies[0].start()
    for d in range(1, n_z):
        back_copies[d - 1].wait_recv()
        copy = spread(d, lax.rem(z - d + n_z, n_z))
        copy.start()
        core_copies.append(copy)
    for copy in core_copies:
        copy.wait_recv()
    gather_slot(5)

    scale = 1.0 / path_count
    ridge = jnp.where(
        lax.broadcasted_iota(jnp.int32, (BLOCK, BLOCK), 0)
        == lax.broadcasted_iota(jnp.int32, (BLOCK, BLOCK), 1), ridge_weight, 0.0,
    )
    for at, (i, j) in enumerate(pairs):
        block = total[at * BLOCK : (at + 1) * BLOCK, :] * scale
        if i == j:
            system[i * BLOCK : (i + 1) * BLOCK, j * BLOCK : (j + 1) * BLOCK] = block + ridge
        else:
            system[i * BLOCK : (i + 1) * BLOCK, j * BLOCK : (j + 1) * BLOCK] = block
            system[j * BLOCK : (j + 1) * BLOCK, i * BLOCK : (i + 1) * BLOCK] = block.T
    moment[...] = jnp.zeros_like(moment)
    for i in range(span):
        moment[0:1, i * BLOCK : (i + 1) * BLOCK] = (
            total[moment_at + i : moment_at + i + 1, :] * scale
        )
    solve(system, moment, inverse, reduced, tile_v, coef, lambda k: gather_slot(6 + k))

    high, middle, low = pieces(coef[0:1, :])
    stack = jnp.concatenate([high, middle, low, jnp.zeros((5, functions), BF16)], axis=0)

    def value_tile(t, carry):
        here = columns(t)
        parts = jnp.dot(stack, basis_v[:, here], preferred_element_type=F32)
        value_v[s, :, here] = parts[0:1] + parts[1:2] + parts[2:3]
        return carry

    lax.fori_loop(0, share_tiles, value_tile, 0)
    value_copies = [
        remote(value_v.at[s], value_v.at[s], v_send.at[r], v_recv.at[r], stock(r))
        for r in range(1, n_s)
    ]
    for copy in value_copies:
        copy.start()
    done = 6 + functions // BLOCK
    gather_slot(done)
    gather_slot(done + 1)
    own_copy.wait()
    shocks_copy.wait()
    for copy in value_copies:
        copy.wait_recv()
    done = done + 2

    def delta_copy(k):
        return pltpu.make_async_copy(
            delta_v.at[:, columns(k)], delta_ref.at[:, columns(k)], delta_sem.at[k]
        )

    def adjoint_tile(k, carry):
        gather_slot(done + 2 * k)
        gather_slot(done + 2 * k + 1)
        if square:
            passed_chunk(2, 1, 2, k).wait_recv()
            passed_chunk(3, 2, 1, k).wait_recv()
        else:
            for r in range(1, n_s):
                own_chunk(r - 1, r, k).wait_recv()
        here = columns(k)
        gathered = whole[:, :, here].reshape(n_s * rows, tile)
        doubled = jnp.concatenate([gathered, gathered], axis=0)
        value = value_v[k // share_tiles, :, columns(lax.rem(k, share_tiles))]
        linear = jnp.dot(split_v[...], doubled, preferred_element_type=F32)
        gains = [exercise_ref[d : d + 1, here].astype(F32) * value for d in range(STEPS)]
        strikes = lax.broadcasted_iota(jnp.int32, (NK, tile), 0).astype(jnp.int16)
        deposit = jnp.zeros(surface_acc.shape, F32)
        for date in range(STEPS - 1, -1, -1):
            at = (STEPS - 1 - date) * rows
            adjoint = linear[at : at + rows]
            for later in range(date, STEPS):
                lift = jnp.concatenate([basket_v[later - date]] * (tile // BLOCK), axis=1)
                adjoint = adjoint + lift * gains[later]
            if date == 0:
                delta_v[:, here] = adjoint
            vega = (adjoint * shocks_v[date, :, here].astype(F32)).astype(BF16)
            spot = bucket_ref[date : date + 1, here].astype(jnp.int16)
            one_hot = jnp.where(spot == strikes, BF16(1), BF16(0))
            deposit = deposit + lax.dot_general(
                vega, one_hot, LANES, preferred_element_type=F32
            )
        surface_acc[...] += deposit
        delta_copy(k).start()
        return carry

    lax.fori_loop(0, chunks, adjoint_tile, 0)

    own_strikes = NK // n_p
    acc_t = surface_acc[...].T
    surface_recv[0] = acc_t.reshape(n_p, own_strikes, rows)
    surface_copies = []
    for d in range(1, n_p):
        other = lax.rem(p + d, n_p)
        surface_copies.append(
            remote(
                surface_recv.at[0, other], surface_recv.at[1, d], s_send.at[d], s_recv.at[d],
                (other, s),
            )
        )
    for copy in surface_copies:
        copy.start()
    for copy in surface_copies:
        copy.wait_recv()
    own = surface_recv[0, p]
    for d in range(1, n_p):
        own = own + surface_recv[1, d]
    surface_ref[...] = own.T

    for copy in surface_copies + value_copies + x_copies + z_copies + back_copies + core_copies:
        copy.wait_send()
    core_copy.wait_send()
    for r in range(1, n_s):
        factor_copy(r).wait_send()

    def drain(k, carry):
        for copy in chunk_copies(k):
            copy.wait_send()
        delta_copy(k).wait()
        return carry

    lax.fori_loop(0, chunks, drain, 0)


def per_device(
    n_p, n_s, prices, loadings, basis_w, basis_bias, payoff, in_fit, cotangent, shocks, corr_gen,
    basket, exercise, bucket,
):
    rows, paths = prices.shape
    rank, functions = basis_w.shape
    share = paths // n_s
    tile = min(TILE, share)
    chunks = paths // tile
    total_rows = sum_rows(functions, n_p)
    n_z = n_p // 2
    kinds = 4 if n_s == 4 else n_s - 1
    vmem = pl.BlockSpec(memory_space=pltpu.VMEM)
    hbm = pl.BlockSpec(memory_space=pl.ANY)
    dma = pltpu.SemaphoreType.DMA
    return pl.pallas_call(
        functools.partial(step_kernel, n_p, n_s, float(paths * n_p)),
        in_specs=[hbm, vmem, vmem, vmem, vmem, vmem, hbm, hbm, vmem, vmem, vmem, vmem],
        out_specs=[hbm, vmem],
        out_shape=[
            jax.ShapeDtypeStruct((rows, paths), F32),
            jax.ShapeDtypeStruct((rows, NK // n_p), F32),
        ],
        scratch_shapes=[
            pltpu.VMEM((rows, paths), BF16),
            pltpu.VMEM((n_s, rows, paths), BF16),
            pltpu.VMEM((STEPS, rows, paths), BF16),
            pltpu.VMEM((rows, paths), F32),
            pltpu.VMEM((n_s, rank, share), F32),
            pltpu.VMEM((n_s, rank, share), F32),
            pltpu.VMEM((functions, 6 * rank + PACK), BF16),
            pltpu.VMEM((functions, share), BF16),
            pltpu.VMEM((total_rows, BLOCK), F32),
            pltpu.VMEM((total_rows // 2, BLOCK), F32),
            pltpu.VMEM((n_z, total_rows // n_p, BLOCK), F32),
            pltpu.VMEM((total_rows // n_p, BLOCK), F32),
            pltpu.VMEM((n_s, total_rows // n_p, BLOCK), F32),
            pltpu.VMEM((total_rows, BLOCK), F32),
            pltpu.VMEM((functions, functions), F32),
            pltpu.VMEM((SUB, functions), F32),
            pltpu.VMEM((functions, BLOCK), F32),
            pltpu.VMEM((functions, functions), F32),
            pltpu.VMEM((BLOCK, BLOCK), F32),
            pltpu.VMEM((SUB, functions), F32),
            pltpu.VMEM((n_s, 1, share), F32),
            pltpu.VMEM((STEPS * rows, 2 * n_s * rows), BF16),
            pltpu.VMEM((STEPS, rows, BLOCK), F32),
            pltpu.VMEM((rows, NK), F32),
            pltpu.VMEM((2, n_p, NK // n_p, rows), F32),
            dma((3,)), dma((chunks,)), dma((n_s,)), dma((n_s,)), dma((kinds, chunks)),
            dma((kinds, chunks)), dma((1,)), dma((1,)), dma((n_z,)), dma((n_z,)), dma((n_s,)),
            dma((n_s,)), dma((n_z,)), dma((n_z,)), dma((n_z,)), dma((n_z,)), dma((n_s,)),
            dma((n_s,)), dma((n_p,)), dma((n_p,)),
        ],
        compiler_params=pltpu.CompilerParams(
            collective_id=0, has_side_effects=True, vmem_limit_bytes=62 * 1024 * 1024
        ),
        name="bermudan_step",
    )(
        prices, loadings, basis_w, basis_bias[None, :], payoff[None, :], in_fit[None, :], cotangent,
        shocks, corr_gen, basket[None, :], exercise, bucket,
    )


def solution(mesh):
    n_p, n_s = mesh.shape["paths"], mesh.shape["stocks"]
    return jax.shard_map(
        functools.partial(per_device, n_p, n_s),
        mesh=mesh,
        in_specs=(
            P("stocks", "paths"),
            P("stocks", None),
            P(),
            P(),
            P("paths"),
            P("paths"),
            P("stocks", "paths"),
            P(None, "stocks", "paths"),
            P(),
            P(),
            P(None, "paths"),
            P(None, "paths"),
        ),
        out_specs=(P("stocks", "paths"), P("stocks", "paths")),
        check_vma=False,
    )
```

```python
import functools

import jax
import jax.numpy as jnp
from jax import lax
from jax.experimental import pallas as pl
from jax.experimental.pallas import tpu as pltpu
from jax.sharding import PartitionSpec as P

NK = 256
STEPS = 4
SUB = 8
BLOCK = 128
PACK = 16
TILE = 1024
EARLY = 1
WIDE = 2
LEVELS = 32767.0

time_step = 0.25
ridge_weight = 0.1
HIGHEST = lax.Precision.HIGHEST
MESH = pl.DeviceIdType.MESH
F32 = jnp.float32
BF16 = jnp.bfloat16
I16 = jnp.int16
LANES = (((1,), (1,)), ((), ()))


def pieces(value):
    high = value.astype(BF16)
    rest = value - high.astype(F32)
    middle = rest.astype(BF16)
    low = (rest - middle.astype(F32)).astype(BF16)
    return high, middle, low


def sweep_block(tile_ref):
    size = tile_ref.shape[0]
    rows = lax.broadcasted_iota(jnp.int32, (SUB, size), 0)
    lanes = lax.broadcasted_iota(jnp.int32, (SUB, size), 1)
    all_lanes = lax.broadcasted_iota(jnp.int32, (size, size), 1)
    for start in range(0, size, SUB):
        whole = tile_ref[...]
        columns = [
            jnp.broadcast_to(whole[:, start + c : start + c + 1], (size, size)) for c in range(SUB)
        ]
        pivots = [columns[c][start : start + SUB] for c in range(SUB)]
        strip = whole[start : start + SUB]
        inside = (lanes >= start) & (lanes < start + SUB)
        strip = jnp.where(inside, jnp.where(lanes - start == rows, 1.0, 0.0), strip)
        for j in range(SUB):
            inverse = 1.0 / pivots[j][j : j + 1]
            chosen = strip[j : j + 1] * inverse
            strip = jnp.where(rows == j, chosen, strip - pivots[j] * chosen)
            for c in range(j + 1, SUB):
                moved = pivots[c][j : j + 1] * inverse
                pivots[c] = jnp.where(rows == j, moved, pivots[c] - pivots[j] * moved)
        inside_all = (all_lanes >= start) & (all_lanes < start + SUB)
        updated = jnp.where(inside_all, 0.0, whole)
        for c in range(SUB):
            updated = updated - columns[c] * strip[c : c + 1]
        tile_ref[...] = updated
        tile_ref[start : start + SUB, :] = strip


def exact_dot(left, right, dims=(((1,), (0,)), ((), ()))):
    return lax.dot_general(
        left, right, dims, preferred_element_type=jnp.float32, precision=HIGHEST
    )


def solve(system_ref, moment_ref, inverse_ref, reduced_ref, tile_ref, out_ref, each):
    size = system_ref.shape[0]
    blocks = size // BLOCK
    for k in range(blocks):
        lo, hi = k * BLOCK, (k + 1) * BLOCK
        each(k)
        tile_ref[...] = system_ref[lo:hi, lo:hi]
        sweep_block(tile_ref)
        inverse = tile_ref[...]
        inverse_ref[lo:hi, :] = inverse
        if hi < size:
            reduced = exact_dot(inverse, system_ref[lo:hi, hi:])
            reduced_ref[lo:hi, hi:] = reduced
            left = jnp.concatenate([system_ref[hi:, lo:hi], moment_ref[:, lo:hi]], axis=0)
            update = exact_dot(left, reduced)
            system_ref[hi:, hi:] -= update[: size - hi]
            moment_ref[:, hi:] -= update[size - hi :]
    for k in range(blocks - 1, -1, -1):
        lo, hi = k * BLOCK, (k + 1) * BLOCK
        found = exact_dot(moment_ref[:, lo:hi], inverse_ref[lo:hi, :])
        if hi < size:
            found = found - exact_dot(out_ref[:, hi:], reduced_ref[lo:hi, hi:], LANES)
        out_ref[:, lo:hi] = found


def levels(value):
    return jnp.round(value).astype(jnp.int32).astype(I16)


def widen(value):
    return value.astype(jnp.int32).astype(F32)


def block_pairs(functions):
    count = functions // BLOCK
    return [(i, j) for i in range(count) for j in range(i + 1)]


def sum_rows(functions, path_devices):
    rows = len(block_pairs(functions)) * BLOCK + functions // BLOCK
    unit = PACK * path_devices
    return -(-rows // unit) * unit


def step_kernel(
    n_p, n_s, path_count,
    prices_ref, loadings_ref, basis_w_ref, bias_ref, payoff_ref, fit_ref, cot_ref, shocks_ref,
    corr_ref, basket_ref, exercise_ref, bucket_ref,
    delta_ref, surface_ref,
    prices_v, whole, shocks_v, delta_v, partial_v, factor_send, factor_recv, range_send, range_recv,
    weights_v, basis_v,
    acc, core_recv, z_piece, z_recv, piece, x_piece, x_recv, total,
    system, moment, inverse, reduced, tile_v, coef, value_v, split_v, basket_v, surface_acc, surface_recv,
    local_sem, delta_sem, f_send, f_recv, g_send, g_recv, ag_send, ag_recv, c1_send, c1_recv, z_send, z_rcv,
    x_send, x_rcv, z4_send, z4_recv, c5_send, c5_recv, v_send, v_recv, s_send, s_recv,
):
    p = lax.axis_index("paths")
    s = lax.axis_index("stocks")
    core = lax.rem(p, 2)
    z = p // 2
    n_z = n_p // 2
    rows, paths = cot_ref.shape
    rank, functions = basis_w_ref.shape
    share = paths // n_s
    tile = min(TILE, share)
    chunks = paths // tile
    share_tiles = share // tile
    square = n_s == 4

    def stock(r):
        return (p, lax.bitwise_xor(s, r))

    def columns(i):
        return pl.ds(pl.multiple_of(i * tile, tile), tile)

    def remote(source, target, send, recv, device):
        return pltpu.make_async_remote_copy(
            src_ref=source, dst_ref=target, send_sem=send, recv_sem=recv,
            device_id=device, device_id_type=MESH,
        )

    prices_copy = pltpu.make_async_copy(prices_ref, prices_v, local_sem.at[0])
    prices_copy.start()

    barrier = pltpu.get_barrier_semaphore()
    for r in range(1, n_s):
        pl.semaphore_signal(barrier, inc=1, device_id=stock(r), device_id_type=MESH)
    for d in range(1, n_p):
        pl.semaphore_signal(
            barrier, inc=1, device_id=(lax.rem(p + d, n_p), s), device_id_type=MESH
        )

    half = rows // 2

    def own_chunk(kind, r, k):
        return remote(
            cot_ref.at[:, columns(k)], whole.at[s, :, columns(k)],
            ag_send.at[kind, k], ag_recv.at[kind, k], stock(r),
        )

    def passed_chunk(kind, source, target, k):
        block = lax.bitwise_xor(s, source)
        part = pl.ds((source - 1) * half, half)
        return remote(
            whole.at[block, part, columns(k)], whole.at[block, part, columns(k)],
            ag_send.at[kind, k], ag_recv.at[kind, k], stock(target),
        )

    def chunk_copies(k):
        if square:
            return [
                own_chunk(0, 1, k), own_chunk(1, 2, k),
                passed_chunk(2, 1, 2, k), passed_chunk(3, 2, 1, k),
            ]
        return [own_chunk(r - 1, r, k) for r in range(1, n_s)]

    def gather_send(k):
        if square:
            own_chunk(0, 1, k).start()
            own_chunk(1, 2, k).start()
        else:
            for r in range(1, n_s):
                own_chunk(r - 1, r, k).start()

    def gather_pass(k):
        if square:
            own_chunk(0, 1, k).wait_recv()
            passed_chunk(2, 1, 2, k).start()
            own_chunk(1, 2, k).wait_recv()
            passed_chunk(3, 2, 1, k).start()

    sent = [0]
    passed = [0]

    def advance(sends, passes):
        for _ in range(min(sends, chunks - sent[0])):
            gather_send(sent[0])
            sent[0] += 1
        for _ in range(min(passes, sent[0] - passed[0])):
            gather_pass(passed[0])
            passed[0] += 1

    pl.semaphore_wait(barrier, n_s + n_p - 2)
    advance(EARLY, 0)

    def factor_copies(r):
        return [
            remote(factor_send.at[r], factor_recv.at[r], f_send.at[r], f_recv.at[r], stock(r)),
            remote(range_send.at[r], range_recv.at[r], g_send.at[r], g_recv.at[r], stock(r)),
        ]

    prices_copy.wait()
    for r in list(range(1, n_s)) + [0]:
        owner = lax.bitwise_xor(s, r)

        def partial(t, largest, owner=owner):
            here = pl.ds(pl.multiple_of(owner * share + t * tile, tile), tile)
            value = lax.dot_general(
                loadings_ref[...], prices_v[:, here], (((1,), (0,)), ((), ())),
                preferred_element_type=F32,
            )
            partial_v[:, columns(t)] = value
            size = jnp.abs(value)
            for c in range(0, tile, BLOCK):
                largest = jnp.maximum(largest, size[:, c : c + BLOCK])
            return largest

        largest = lax.fori_loop(0, share_tiles, partial, jnp.zeros((rank, BLOCK), F32))
        if r > 0:
            top = jnp.maximum(jnp.max(largest, axis=1, keepdims=True), 1e-30)
            range_send[r] = jnp.broadcast_to(top * (1.0 / LEVELS), (rank, BLOCK))
            steps = LEVELS / top

            def quantize(t, carry, r=r, steps=steps):
                factor_send[r, :, columns(t)] = levels(partial_v[:, columns(t)] * steps)
                return carry

            lax.fori_loop(0, share_tiles, quantize, 0)
            for copy in factor_copies(r):
                copy.start()

    advance(3, 0)
    own_copy = pltpu.make_async_copy(cot_ref, whole.at[s], local_sem.at[1])
    own_copy.start()
    shocks_copy = pltpu.make_async_copy(shocks_ref, shocks_v, local_sem.at[2])
    shocks_copy.start()

    weight_parts = pieces(basis_w_ref[...])
    bias_parts = pieces(bias_ref[...])
    packed = [weight_parts[i] for i in (0, 0, 1, 0, 1, 2)]
    spare = jnp.zeros((PACK - 3, functions), F32)
    tail = jnp.concatenate([part.astype(F32) for part in bias_parts] + [spare], axis=0)
    stacked = jnp.concatenate([part.astype(F32) for part in packed] + [tail], axis=0)
    weights_v[...] = stacked.T.astype(BF16)
    acc[...] = jnp.zeros_like(acc)
    surface_acc[...] = jnp.zeros_like(surface_acc)

    step = time_step * corr_ref[...].astype(F32)
    own_rows = pl.ds(pl.multiple_of(s * rows, rows), rows)
    own_step = time_step * corr_ref[own_rows, :].astype(F32)
    own_basket = jnp.sum(
        jnp.where(
            lax.broadcasted_iota(jnp.int32, own_step.shape, 1)
            == lax.broadcasted_iota(jnp.int32, own_step.shape, 0) + s * rows,
            basket_ref[...], 0.0,
        ), axis=1, keepdims=True,
    )
    power = own_step
    rest = jnp.zeros_like(own_step)
    split_v[0:rows, :] = own_step.astype(BF16)
    basket_v[0] = jnp.broadcast_to(own_basket, basket_v.shape[1:])
    for k in range(1, STEPS):
        basket_v[k] = jnp.broadcast_to(
            own_basket + jnp.sum(power * basket_ref[...], axis=1, keepdims=True),
            basket_v.shape[1:],
        )
        moved = jnp.dot(power, step, preferred_element_type=F32, precision=HIGHEST)
        power = power + own_step + moved
        rest = rest + moved
        split_v[k * rows : (k + 1) * rows, :] = rest.astype(BF16)

    for r in range(1, n_s):
        for copy in factor_copies(r):
            copy.wait_recv()
    pairs = block_pairs(functions)
    span = functions // BLOCK
    moment_at = len(pairs) * BLOCK
    share_start = s * share
    wide = 2 * BLOCK

    def basis_tile(t, carry):
        here = columns(t)
        factors = partial_v[:, here]
        for r in range(1, n_s):
            unit = jnp.concatenate([range_recv[r]] * (tile // BLOCK), axis=1)
            factors = factors + widen(factor_recv[r, :, here]) * unit
        high, middle, low = pieces(factors)
        ones = jnp.where(
            lax.broadcasted_iota(jnp.int32, (PACK, tile), 0) < 3, 1.0, 0.0
        ).astype(BF16)
        packed_factors = jnp.concatenate([high, middle, high, low, middle, high, ones], axis=0)
        raised = jnp.dot(weights_v[...], packed_factors, preferred_element_type=F32)
        basis = jnp.tanh(raised).astype(BF16)
        basis_v[:, here] = basis
        from_start = pl.ds(pl.multiple_of(share_start + t * tile, tile), tile)
        picked = basis * fit_ref[:, from_start].astype(BF16)
        for i in range(0, span, 2):
            count = min(2, span - i)
            for j in range(0, i + 1, 2):
                part = lax.dot_general(
                    basis[i * BLOCK : (i + count) * BLOCK],
                    picked[j * BLOCK : min(j + 2, span) * BLOCK],
                    LANES, preferred_element_type=F32,
                )
                for a in range(count):
                    for b in range(min(2, span - j)):
                        if (i + a, j + b) in pairs:
                            at = pairs.index((i + a, j + b)) * BLOCK
                            acc[at : at + BLOCK, :] += part[
                                a * BLOCK : (a + 1) * BLOCK, b * BLOCK : (b + 1) * BLOCK
                            ]
        cash_rows = payoff_ref[
            pl.ds(pl.multiple_of((share_start + t * tile) // BLOCK, SUB), tile // BLOCK), :
        ].astype(F32)
        cash_row = jnp.concatenate(
            [cash_rows[i : i + 1, :] for i in range(tile // BLOCK)], axis=1
        ).astype(BF16)
        cash = jnp.broadcast_to(cash_row, (2 * SUB, tile))
        cash_sum = lax.dot_general(cash, picked, LANES, preferred_element_type=F32)
        for i in range(span):
            acc[moment_at + i : moment_at + i + 1, :] += cash_sum[
                0:1, i * BLOCK : (i + 1) * BLOCK
            ]
        return carry

    lax.fori_loop(0, share_tiles, basis_tile, 0)
    advance(1, 0)

    half_rows = acc.shape[0] // 2
    piece_rows = acc.shape[0] // n_p
    partner = (p + 1 - 2 * core, s)

    def half_at(c):
        return pl.ds(pl.multiple_of(c * half_rows, SUB), half_rows)

    def piece_at(c, zz):
        return pl.ds(pl.multiple_of(c * half_rows + zz * piece_rows, SUB), piece_rows)

    def z_peer(d):
        other = lax.rem(z + d, n_z)
        return other, (2 * other + core, s)

    def level_rows(count):
        def rows_of(c, zz):
            at = c * half_rows + zz * piece_rows + lax.broadcasted_iota(
                jnp.int32, (piece_rows, BLOCK), 0
            )
            return jnp.where(at < moment_at, LEVELS / count, LEVELS / (4.0 * count))

        return rows_of

    core_copy = remote(
        acc.at[half_at(1 - core)], core_recv, c1_send.at[0], c1_recv.at[0], partner
    )
    core_copy.start()
    core_copy.wait_recv()
    chip_scale = level_rows(2 * share)
    for zz in range(n_z):
        both = acc[piece_at(core, zz), :] + core_recv[zz * piece_rows : (zz + 1) * piece_rows, :]
        acc[piece_at(core, zz), :] = both
        z_piece[zz] = levels(both * chip_scale(core, zz))
    z_copies = []
    for d in range(1, n_z):
        other, device = z_peer(d)
        z_copies.append(
            remote(z_piece.at[other], z_recv.at[d], z_send.at[d], z_rcv.at[d], device)
        )
    for copy in z_copies:
        copy.start()
    advance(0, 2)
    for copy in z_copies:
        copy.wait_recv()
    mine = acc[piece_at(core, z), :]
    grain = 1.0 / level_rows(2 * share)(core, z)
    for d in range(1, n_z):
        mine = mine + widen(z_recv[d]) * grain
    piece[...] = mine
    x_piece[...] = levels(mine * level_rows(n_p * share)(core, z))
    x_copies = [
        remote(x_piece, x_recv.at[r], x_send.at[r], x_rcv.at[r], stock(r)) for r in range(1, n_s)
    ]
    for copy in x_copies:
        copy.start()
    advance(3, 1)
    for copy in x_copies:
        copy.wait_recv()
    mine = piece[...]
    grain = 1.0 / level_rows(n_p * share)(core, z)
    for r in range(1, n_s):
        mine = mine + widen(x_recv[r]) * grain
    total[piece_at(core, z), :] = mine

    def spread(slot, zz):
        return remote(
            total.at[piece_at(core, zz)], total.at[piece_at(core, zz)],
            c5_send.at[slot], c5_recv.at[slot], partner,
        )

    back_copies = []
    for d in range(1, n_z):
        _, device = z_peer(d)
        back_copies.append(
            remote(
                total.at[piece_at(core, z)], total.at[piece_at(core, z)],
                z4_send.at[d], z4_recv.at[d], device,
            )
        )
    for copy in back_copies:
        copy.start()
    core_copies = [spread(0, z)]
    core_copies[0].start()
    for d in range(1, n_z):
        back_copies[d - 1].wait_recv()
        copy = spread(d, lax.rem(z - d + n_z, n_z))
        copy.start()
        core_copies.append(copy)
    for copy in core_copies:
        copy.wait_recv()
    advance(1, 2)

    scale = 1.0 / path_count
    ridge = jnp.where(
        lax.broadcasted_iota(jnp.int32, (BLOCK, BLOCK), 0)
        == lax.broadcasted_iota(jnp.int32, (BLOCK, BLOCK), 1), ridge_weight, 0.0,
    )
    for at, (i, j) in enumerate(pairs):
        block = total[at * BLOCK : (at + 1) * BLOCK, :] * scale
        if i == j:
            system[i * BLOCK : (i + 1) * BLOCK, j * BLOCK : (j + 1) * BLOCK] = block + ridge
        else:
            system[i * BLOCK : (i + 1) * BLOCK, j * BLOCK : (j + 1) * BLOCK] = block
            system[j * BLOCK : (j + 1) * BLOCK, i * BLOCK : (i + 1) * BLOCK] = block.T
    moment[...] = jnp.zeros_like(moment)
    for i in range(span):
        moment[0:1, i * BLOCK : (i + 1) * BLOCK] = (
            total[moment_at + i : moment_at + i + 1, :] * scale
        )
    solve_sent, solve_passed = sent[0], passed[0]
    solve_steps = functions // BLOCK

    def during_solve(k):
        gather_send(solve_sent + k)
        gather_pass(solve_passed + k)

    solve(system, moment, inverse, reduced, tile_v, coef, during_solve)
    sent[0] += solve_steps
    passed[0] += solve_steps

    high, middle, low = pieces(coef[0:1, :])
    stack = jnp.concatenate([high, middle, low, jnp.zeros((5, functions), BF16)], axis=0)

    def value_tile(t, carry):
        here = columns(t)
        parts = jnp.dot(stack, basis_v[:, here], preferred_element_type=F32)
        value_v[s, :, here] = parts[0:1] + parts[1:2] + parts[2:3]
        return carry

    lax.fori_loop(0, share_tiles, value_tile, 0)
    value_copies = [
        remote(value_v.at[s], value_v.at[s], v_send.at[r], v_recv.at[r], stock(r))
        for r in range(1, n_s)
    ]
    for copy in value_copies:
        copy.start()
    advance(2, 2)
    own_copy.wait()
    shocks_copy.wait()
    for copy in value_copies:
        copy.wait_recv()
    advance(chunks, 0)
    first_left = passed[0]
    ahead = 2 + WIDE
    wide_tiles = share_tiles // WIDE

    def wide_columns(k):
        return pl.ds(pl.multiple_of(k * WIDE * tile, WIDE * tile), WIDE * tile)

    def delta_copy(k):
        return pltpu.make_async_copy(
            delta_v.at[:, wide_columns(k)], delta_ref.at[:, wide_columns(k)], delta_sem.at[k]
        )

    def adjoint_tile(k, carry):
        for c in range(WIDE):
            chunk = k * WIDE + c
            if square:
                ready = chunk + ahead

                @pl.when(jnp.logical_and(ready >= first_left, ready < chunks))
                def _():
                    gather_pass(ready)

        for c in range(WIDE):
            chunk = k * WIDE + c
            if square:
                passed_chunk(2, 1, 2, chunk).wait_recv()
                passed_chunk(3, 2, 1, chunk).wait_recv()
            else:
                for r in range(1, n_s):
                    own_chunk(r - 1, r, chunk).wait_recv()
        width = WIDE * tile
        here = pl.ds(pl.multiple_of(k * width, width), width)
        gathered = whole[:, :, here].reshape(n_s * rows, width)
        value = value_v[
            k // wide_tiles, :, pl.ds(pl.multiple_of(lax.rem(k, wide_tiles) * width, width), width)
        ]
        mixed = jnp.dot(split_v[...], gathered, preferred_element_type=F32)
        linear = whole[s, :, here].astype(F32)
        gains = [exercise_ref[d : d + 1, here].astype(F32) * value for d in range(STEPS)]
        strikes = lax.broadcasted_iota(jnp.int32, (BLOCK, width), 0).astype(jnp.int16)
        deposit = jnp.zeros(surface_acc.shape, F32)
        for date in range(STEPS - 1, -1, -1):
            at = (STEPS - 1 - date) * rows
            linear = linear + mixed[0:rows]
            adjoint = linear if at == 0 else linear + mixed[at : at + rows]
            for later in range(date, STEPS):
                lift = jnp.concatenate([basket_v[later - date]] * (width // BLOCK), axis=1)
                adjoint = adjoint + lift * gains[later]
            if date == 0:
                delta_v[:, here] = adjoint
            vega = (adjoint * shocks_v[date, :, here].astype(F32)).astype(BF16)
            bucket = bucket_ref[date : date + 1, here]
            spot = (bucket % BLOCK).astype(jnp.int16)
            group = (bucket // BLOCK).astype(jnp.int16)
            one_hot = jnp.where(spot == strikes, BF16(1), BF16(0))
            grouped = jnp.concatenate(
                [jnp.where(group == g, vega, BF16(0)) for g in range(NK // BLOCK)], axis=0
            )
            deposit = deposit + lax.dot_general(
                one_hot, grouped, LANES, preferred_element_type=F32
            )
        surface_acc[...] += deposit
        delta_copy(k).start()
        return carry

    for k in range(first_left, min(ahead, chunks)):
        gather_pass(k)
    lax.fori_loop(0, chunks // WIDE, adjoint_tile, 0)

    own_strikes = NK // n_p
    surface_recv[0] = jnp.concatenate(
        [surface_acc[:, g * rows : (g + 1) * rows] for g in range(NK // BLOCK)], axis=0
    ).reshape(n_p, own_strikes, rows)
    surface_copies = []
    for d in range(1, n_p):
        other = lax.rem(p + d, n_p)
        surface_copies.append(
            remote(
                surface_recv.at[0, other], surface_recv.at[1, d], s_send.at[d], s_recv.at[d],
                (other, s),
            )
        )
    for copy in surface_copies:
        copy.start()
    for copy in surface_copies:
        copy.wait_recv()
    own = surface_recv[0, p]
    for d in range(1, n_p):
        own = own + surface_recv[1, d]
    surface_ref[...] = own

    for copy in surface_copies + value_copies + x_copies + z_copies + back_copies + core_copies:
        copy.wait_send()
    core_copy.wait_send()
    for r in range(1, n_s):
        for copy in factor_copies(r):
            copy.wait_send()

    def drain(k, carry):
        for copy in chunk_copies(k):
            copy.wait_send()
        return carry

    lax.fori_loop(0, chunks, drain, 0)
    for k in range(chunks // WIDE):
        delta_copy(k).wait()


def per_device(
    n_p, n_s, prices, loadings, basis_w, basis_bias, payoff, in_fit, cotangent, shocks, corr_gen,
    basket, exercise, bucket,
):
    rows, paths = prices.shape
    rank, functions = basis_w.shape
    share = paths // n_s
    tile = min(TILE, share)
    chunks = paths // tile
    total_rows = sum_rows(functions, n_p)
    n_z = n_p // 2
    kinds = 4 if n_s == 4 else n_s - 1
    vmem = pl.BlockSpec(memory_space=pltpu.VMEM)
    hbm = pl.BlockSpec(memory_space=pl.ANY)
    dma = pltpu.SemaphoreType.DMA
    delta, surface = pl.pallas_call(
        functools.partial(step_kernel, n_p, n_s, float(paths * n_p)),
        in_specs=[hbm, vmem, vmem, vmem, vmem, vmem, hbm, hbm, vmem, vmem, vmem, vmem],
        out_specs=[hbm, vmem],
        out_shape=[
            jax.ShapeDtypeStruct((rows, paths), F32),
            jax.ShapeDtypeStruct((NK // n_p, rows), F32),
        ],
        scratch_shapes=[
            pltpu.VMEM((rows, paths), BF16),
            pltpu.VMEM((n_s, rows, paths), BF16),
            pltpu.VMEM((STEPS, rows, paths), BF16),
            pltpu.VMEM((rows, paths), F32),
            pltpu.VMEM((rank, share), F32),
            pltpu.VMEM((n_s, rank, share), I16),
            pltpu.VMEM((n_s, rank, share), I16),
            pltpu.VMEM((n_s, rank, BLOCK), F32),
            pltpu.VMEM((n_s, rank, BLOCK), F32),
            pltpu.VMEM((functions, 6 * rank + PACK), BF16),
            pltpu.VMEM((functions, share), BF16),
            pltpu.VMEM((total_rows, BLOCK), F32),
            pltpu.VMEM((total_rows // 2, BLOCK), F32),
            pltpu.VMEM((n_z, total_rows // n_p, BLOCK), I16),
            pltpu.VMEM((n_z, total_rows // n_p, BLOCK), I16),
            pltpu.VMEM((total_rows // n_p, BLOCK), F32),
            pltpu.VMEM((total_rows // n_p, BLOCK), I16),
            pltpu.VMEM((n_s, total_rows // n_p, BLOCK), I16),
            pltpu.VMEM((total_rows, BLOCK), F32),
            pltpu.VMEM((functions, functions), F32),
            pltpu.VMEM((SUB, functions), F32),
            pltpu.VMEM((functions, BLOCK), F32),
            pltpu.VMEM((functions, functions), F32),
            pltpu.VMEM((BLOCK, BLOCK), F32),
            pltpu.VMEM((SUB, functions), F32),
            pltpu.VMEM((n_s, 1, share), F32),
            pltpu.VMEM((STEPS * rows, n_s * rows), BF16),
            pltpu.VMEM((STEPS, rows, BLOCK), F32),
            pltpu.VMEM((BLOCK, NK // BLOCK * rows), F32),
            pltpu.VMEM((2, n_p, NK // n_p, rows), F32),
            dma((3,)), dma((chunks,)), dma((n_s,)), dma((n_s,)), dma((n_s,)), dma((n_s,)),
            dma((kinds, chunks)),
            dma((kinds, chunks)), dma((1,)), dma((1,)), dma((n_z,)), dma((n_z,)), dma((n_s,)),
            dma((n_s,)), dma((n_z,)), dma((n_z,)), dma((n_z,)), dma((n_z,)), dma((n_s,)),
            dma((n_s,)), dma((n_p,)), dma((n_p,)),
        ],
        compiler_params=pltpu.CompilerParams(
            collective_id=0, has_side_effects=True, vmem_limit_bytes=62 * 1024 * 1024
        ),
        name="bermudan_step",
    )(
        prices, loadings.T, basis_w, basis_bias[None, :], payoff.reshape(-1, BLOCK), in_fit[None, :], cotangent,
        shocks, corr_gen, basket[None, :], exercise, bucket,
    )
    return delta, surface.T


def solution(mesh):
    n_p, n_s = mesh.shape["paths"], mesh.shape["stocks"]
    return jax.shard_map(
        functools.partial(per_device, n_p, n_s),
        mesh=mesh,
        in_specs=(
            P("stocks", "paths"),
            P("stocks", None),
            P(),
            P(),
            P("paths"),
            P("paths"),
            P("stocks", "paths"),
            P(None, "stocks", "paths"),
            P(),
            P(),
            P(None, "paths"),
            P(None, "paths"),
        ),
        out_specs=(P("stocks", "paths"), P("stocks", "paths")),
        check_vma=False,
    )
```

```python
import functools

import jax
import jax.numpy as jnp
from jax import lax
from jax.experimental import pallas as pl
from jax.experimental.pallas import tpu as pltpu
from jax.sharding import PartitionSpec as P

NK = 256
STEPS = 4
SUB = 8
BLOCK = 128
PACK = 16
TILE = 1024
EARLY = 1
GAP = 0
AFTER = 3
WIDE = 2
LEVELS = 32767.0

time_step = 0.25
ridge_weight = 0.1
HIGHEST = lax.Precision.HIGHEST
MESH = pl.DeviceIdType.MESH
F32 = jnp.float32
BF16 = jnp.bfloat16
I16 = jnp.int16
LANES = (((1,), (1,)), ((), ()))


def pieces(value):
    high = value.astype(BF16)
    rest = value - high.astype(F32)
    middle = rest.astype(BF16)
    low = (rest - middle.astype(F32)).astype(BF16)
    return high, middle, low


def sweep_block(tile_ref):
    size = tile_ref.shape[0]
    rows = lax.broadcasted_iota(jnp.int32, (SUB, size), 0)
    lanes = lax.broadcasted_iota(jnp.int32, (SUB, size), 1)
    all_lanes = lax.broadcasted_iota(jnp.int32, (size, size), 1)
    for start in range(0, size, SUB):
        whole = tile_ref[...]
        columns = [
            jnp.broadcast_to(whole[:, start + c : start + c + 1], (size, size)) for c in range(SUB)
        ]
        pivots = [columns[c][start : start + SUB] for c in range(SUB)]
        strip = whole[start : start + SUB]
        inside = (lanes >= start) & (lanes < start + SUB)
        strip = jnp.where(inside, jnp.where(lanes - start == rows, 1.0, 0.0), strip)
        for j in range(SUB):
            inverse = 1.0 / pivots[j][j : j + 1]
            chosen = strip[j : j + 1] * inverse
            strip = jnp.where(rows == j, chosen, strip - pivots[j] * chosen)
            for c in range(j + 1, SUB):
                moved = pivots[c][j : j + 1] * inverse
                pivots[c] = jnp.where(rows == j, moved, pivots[c] - pivots[j] * moved)
        inside_all = (all_lanes >= start) & (all_lanes < start + SUB)
        updated = jnp.where(inside_all, 0.0, whole)
        for c in range(SUB):
            updated = updated - columns[c] * strip[c : c + 1]
        tile_ref[...] = updated
        tile_ref[start : start + SUB, :] = strip


def exact_dot(left, right, dims=(((1,), (0,)), ((), ()))):
    return lax.dot_general(
        left, right, dims, preferred_element_type=jnp.float32, precision=HIGHEST
    )


def solve(system_ref, moment_ref, inverse_ref, reduced_ref, tile_ref, out_ref, each):
    size = system_ref.shape[0]
    blocks = size // BLOCK
    for k in range(blocks):
        lo, hi = k * BLOCK, (k + 1) * BLOCK
        each(k)
        tile_ref[...] = system_ref[lo:hi, lo:hi]
        sweep_block(tile_ref)
        inverse = tile_ref[...]
        inverse_ref[lo:hi, :] = inverse
        if hi < size:
            reduced = exact_dot(inverse, system_ref[lo:hi, hi:])
            reduced_ref[lo:hi, hi:] = reduced
            left = jnp.concatenate([system_ref[hi:, lo:hi], moment_ref[:, lo:hi]], axis=0)
            update = exact_dot(left, reduced)
            system_ref[hi:, hi:] -= update[: size - hi]
            moment_ref[:, hi:] -= update[size - hi :]
    for k in range(blocks - 1, -1, -1):
        lo, hi = k * BLOCK, (k + 1) * BLOCK
        found = exact_dot(moment_ref[:, lo:hi], inverse_ref[lo:hi, :])
        if hi < size:
            found = found - exact_dot(out_ref[:, hi:], reduced_ref[lo:hi, hi:], LANES)
        out_ref[:, lo:hi] = found


def levels(value):
    return jnp.round(value).astype(jnp.int32).astype(I16)


def widen(value):
    return value.astype(jnp.int32).astype(F32)


def block_pairs(functions):
    count = functions // BLOCK
    return [(i, j) for i in range(count) for j in range(i + 1)]


def sum_rows(functions, path_devices):
    rows = len(block_pairs(functions)) * BLOCK + functions // BLOCK
    unit = PACK * path_devices
    return -(-rows // unit) * unit


def step_kernel(
    n_p, n_s, path_count,
    prices_ref, loadings_in, basis_w_in, bias_in, payoff_in, fit_in, cot_ref, shocks_ref,
    corr_in, basket_in, exercise_in, bucket_in,
    delta_ref, surface_ref,
    loadings_ref, basis_w_ref, bias_ref, payoff_ref, fit_ref, corr_ref, basket_ref, exercise_ref,
    bucket_ref,
    prices_v, whole, shocks_v, delta_v, partial_v, factor_send, factor_recv, range_send, range_recv,
    weights_v, basis_v,
    acc, core_recv, z_piece, z_recv, piece, x_piece, x_recv, total,
    system, moment, inverse, reduced, tile_v, coef, value_v, split_v, basket_v, surface_acc, surface_recv,
    local_sem, delta_sem, f_send, f_recv, g_send, g_recv, ag_send, ag_recv, c1_send, c1_recv, z_send, z_rcv,
    x_send, x_rcv, z4_send, z4_recv, c5_send, c5_recv, v_send, v_recv, s_send, s_recv,
):
    p = lax.axis_index("paths")
    s = lax.axis_index("stocks")
    core = lax.rem(p, 2)
    z = p // 2
    n_z = n_p // 2
    rows, paths = cot_ref.shape
    rank, functions = basis_w_ref.shape
    share = paths // n_s
    tile = min(TILE, share)
    chunks = paths // tile
    share_tiles = share // tile
    square = n_s == 4

    def stock(r):
        return (p, lax.bitwise_xor(s, r))

    def columns(i):
        return pl.ds(pl.multiple_of(i * tile, tile), tile)

    def remote(source, target, send, recv, device):
        return pltpu.make_async_remote_copy(
            src_ref=source, dst_ref=target, send_sem=send, recv_sem=recv,
            device_id=device, device_id_type=MESH,
        )

    barrier = pltpu.get_barrier_semaphore()
    for r in range(1, n_s):
        pl.semaphore_signal(barrier, inc=1, device_id=stock(r), device_id_type=MESH)
    for d in range(1, n_p):
        pl.semaphore_signal(
            barrier, inc=1, device_id=(lax.rem(p + d, n_p), s), device_id_type=MESH
        )
    loadings_copy = pltpu.make_async_copy(loadings_in, loadings_ref, local_sem.at[3])
    loadings_copy.start()
    prices_copy = pltpu.make_async_copy(prices_ref, prices_v, local_sem.at[0])
    prices_copy.start()
    small_copies = [
        pltpu.make_async_copy(source, target, local_sem.at[4 + i])
        for i, (source, target) in enumerate([
            (basis_w_in, basis_w_ref), (bias_in, bias_ref), (corr_in, corr_ref),
            (basket_in, basket_ref), (payoff_in, payoff_ref), (fit_in, fit_ref),
            (exercise_in, exercise_ref), (bucket_in, bucket_ref),
        ])
    ]

    half = rows // 2

    def own_chunk(kind, r, k):
        return remote(
            cot_ref.at[:, columns(k)], whole.at[s, :, columns(k)],
            ag_send.at[kind, k], ag_recv.at[kind, k], stock(r),
        )

    def passed_chunk(kind, source, target, k):
        block = lax.bitwise_xor(s, source)
        part = pl.ds((source - 1) * half, half)
        return remote(
            whole.at[block, part, columns(k)], whole.at[block, part, columns(k)],
            ag_send.at[kind, k], ag_recv.at[kind, k], stock(target),
        )

    def chunk_copies(k):
        if square:
            return [
                own_chunk(0, 1, k), own_chunk(1, 2, k),
                passed_chunk(2, 1, 2, k), passed_chunk(3, 2, 1, k),
            ]
        return [own_chunk(r - 1, r, k) for r in range(1, n_s)]

    def gather_send(k):
        if square:
            own_chunk(0, 1, k).start()
            own_chunk(1, 2, k).start()
        else:
            for r in range(1, n_s):
                own_chunk(r - 1, r, k).start()

    def gather_pass(k):
        if square:
            own_chunk(0, 1, k).wait_recv()
            passed_chunk(2, 1, 2, k).start()
            own_chunk(1, 2, k).wait_recv()
            passed_chunk(3, 2, 1, k).start()

    sent = [0]
    passed = [0]

    def advance(sends, passes):
        for _ in range(min(sends, chunks - sent[0])):
            gather_send(sent[0])
            sent[0] += 1
        for _ in range(min(passes, sent[0] - passed[0])):
            gather_pass(passed[0])
            passed[0] += 1

    pl.semaphore_wait(barrier, n_s + n_p - 2)
    advance(EARLY, 0)

    half_share = share // 2
    half_tile = min(tile, half_share)

    def part_at(owner, h, t):
        at = owner * share + h * half_share + t * half_tile
        return pl.ds(pl.multiple_of(at, half_tile), half_tile)

    def half_at_tile(h, t):
        return pl.ds(pl.multiple_of(h * half_share + t * half_tile, half_tile), half_tile)

    def send_levels(slot):
        def top_of(largest):
            top = jnp.maximum(jnp.max(largest, axis=1, keepdims=True), 1e-30)
            range_send[slot] = jnp.broadcast_to(top * (1.0 / LEVELS), (rank, BLOCK))
            return LEVELS / top

        return top_of

    def grow(largest, value):
        size = jnp.abs(value)
        for c in range(0, half_tile, BLOCK):
            largest = jnp.maximum(largest, size[:, c : c + BLOCK])
        return largest

    def partial_half(r, h):
        owner = lax.bitwise_xor(s, r)

        def run(t, largest):
            value = lax.dot_general(
                loadings_ref[...], prices_v[:, part_at(owner, h, t)], (((1,), (0,)), ((), ())),
                preferred_element_type=F32,
            )
            partial_v[r, :, half_at_tile(h, t)] = value
            return grow(largest, value)

        return lax.fori_loop(0, half_share // half_tile, run, jnp.zeros((rank, BLOCK), F32))

    def quantize_half(slot, r, h, largest):
        steps = send_levels(slot)(largest)

        def run(t, carry):
            here = half_at_tile(h, t)
            there = pl.ds(pl.multiple_of(t * half_tile, half_tile), half_tile)
            factor_send[slot, :, there] = levels(partial_v[r, :, here] * steps)
            return carry

        lax.fori_loop(0, half_share // half_tile, run, 0)

    def factor_copies(slot, device):
        return [
            remote(
                factor_send.at[slot], factor_recv.at[slot], f_send.at[slot], f_recv.at[slot], device
            ),
            remote(
                range_send.at[slot], range_recv.at[slot], g_send.at[slot], g_recv.at[slot], device
            ),
        ]

    def add_half(slot, r, h):
        unit = jnp.concatenate([range_recv[slot]] * (half_tile // BLOCK), axis=1)

        def run(t, largest):
            here = half_at_tile(h, t)
            there = pl.ds(pl.multiple_of(t * half_tile, half_tile), half_tile)
            value = partial_v[r, :, here] + widen(factor_recv[slot, :, there]) * unit
            partial_v[r, :, here] = value
            return grow(largest, value)

        return lax.fori_loop(0, half_share // half_tile, run, jnp.zeros((rank, BLOCK), F32))

    loadings_copy.wait()
    prices_copy.wait()
    for copy in small_copies:
        copy.start()
    factor_sends = []
    if square:
        first_steps = [(0, 3, 0, 1), (1, 3, 1, 2), (2, 1, 0, 1), (3, 2, 1, 2)]
        for slot, r, h, neighbour in first_steps:
            quantize_half(slot, r, h, partial_half(r, h))
            copies = factor_copies(slot, stock(neighbour))
            for copy in copies:
                copy.start()
            factor_sends.append(copies)
        for r, h in ((2, 0), (1, 1), (0, 0), (0, 1)):
            partial_half(r, h)
    else:
        for r in range(1, n_s):
            for h in range(2):
                slot = 2 * (r - 1) + h
                quantize_half(slot, r, h, partial_half(r, h))
                copies = factor_copies(slot, stock(r))
                for copy in copies:
                    copy.start()
                factor_sends.append(copies)
        for h in range(2):
            partial_half(0, h)

    advance(GAP, 0)
    own_copy = pltpu.make_async_copy(cot_ref, whole.at[s], local_sem.at[1])
    own_copy.start()
    shocks_copy = pltpu.make_async_copy(shocks_ref, shocks_v, local_sem.at[2])
    shocks_copy.start()

    for copy in small_copies:
        copy.wait()
    weight_parts = pieces(basis_w_ref[...])
    bias_parts = pieces(bias_ref[...])
    packed = [weight_parts[i] for i in (0, 0, 1, 0, 1, 2)]
    spare = jnp.zeros((PACK - 3, functions), F32)
    tail = jnp.concatenate([part.astype(F32) for part in bias_parts] + [spare], axis=0)
    stacked = jnp.concatenate([part.astype(F32) for part in packed] + [tail], axis=0)
    weights_v[...] = stacked.T.astype(BF16)
    acc[...] = jnp.zeros_like(acc)
    surface_acc[...] = jnp.zeros_like(surface_acc)

    step = time_step * corr_ref[...].astype(F32)
    own_rows = pl.ds(pl.multiple_of(s * rows, rows), rows)
    own_step = time_step * corr_ref[own_rows, :].astype(F32)
    own_basket = jnp.sum(
        jnp.where(
            lax.broadcasted_iota(jnp.int32, own_step.shape, 1)
            == lax.broadcasted_iota(jnp.int32, own_step.shape, 0) + s * rows,
            basket_ref[...], 0.0,
        ), axis=1, keepdims=True,
    )
    power = own_step
    rest = jnp.zeros_like(own_step)
    split_v[0:rows, :] = own_step.astype(BF16)
    basket_v[0] = jnp.broadcast_to(own_basket, basket_v.shape[1:])
    for k in range(1, STEPS):
        basket_v[k] = jnp.broadcast_to(
            own_basket + jnp.sum(power * basket_ref[...], axis=1, keepdims=True),
            basket_v.shape[1:],
        )
        moved = jnp.dot(power, step, preferred_element_type=F32, precision=HIGHEST)
        power = power + own_step + moved
        rest = rest + moved
        split_v[k * rows : (k + 1) * rows, :] = rest.astype(BF16)

    if square:
        for slot, r, h, neighbour in ((0, 2, 0, 2), (1, 1, 1, 1)):
            for copy in factor_sends[slot]:
                copy.wait_recv()
            quantize_half(4 + slot, r, h, add_half(slot, r, h))
            copies = factor_copies(4 + slot, stock(neighbour))
            for copy in copies:
                copy.start()
            factor_sends.append(copies)
        advance(AFTER, 0)
        arrivals = [(2, 0), (3, 1), (4, 0), (5, 1)]
    else:
        arrivals = [(2 * (r - 1) + h, h) for r in range(1, n_s) for h in range(2)]
    for slot, h in arrivals:
        for copy in factor_sends[slot]:
            copy.wait_recv()
        add_half(slot, 0, h)
    pairs = block_pairs(functions)
    span = functions // BLOCK
    moment_at = len(pairs) * BLOCK
    share_start = s * share
    wide = 2 * BLOCK

    def basis_tile(t, carry):
        here = columns(t)
        factors = partial_v[0, :, here]
        high, middle, low = pieces(factors)
        ones = jnp.where(
            lax.broadcasted_iota(jnp.int32, (PACK, tile), 0) < 3, 1.0, 0.0
        ).astype(BF16)
        packed_factors = jnp.concatenate([high, middle, high, low, middle, high, ones], axis=0)
        raised = jnp.dot(weights_v[...], packed_factors, preferred_element_type=F32)
        basis = jnp.tanh(raised).astype(BF16)
        basis_v[:, here] = basis
        from_start = pl.ds(pl.multiple_of(share_start + t * tile, tile), tile)
        picked = basis * fit_ref[:, from_start].astype(BF16)
        for i in range(0, span, 2):
            count = min(2, span - i)
            for j in range(0, i + 1, 2):
                part = lax.dot_general(
                    basis[i * BLOCK : (i + count) * BLOCK],
                    picked[j * BLOCK : min(j + 2, span) * BLOCK],
                    LANES, preferred_element_type=F32,
                )
                for a in range(count):
                    for b in range(min(2, span - j)):
                        if (i + a, j + b) in pairs:
                            at = pairs.index((i + a, j + b)) * BLOCK
                            acc[at : at + BLOCK, :] += part[
                                a * BLOCK : (a + 1) * BLOCK, b * BLOCK : (b + 1) * BLOCK
                            ]
        cash_rows = payoff_ref[
            pl.ds(pl.multiple_of((share_start + t * tile) // BLOCK, SUB), tile // BLOCK), :
        ].astype(F32)
        cash_row = jnp.concatenate(
            [cash_rows[i : i + 1, :] for i in range(tile // BLOCK)], axis=1
        ).astype(BF16)
        cash = jnp.broadcast_to(cash_row, (2 * SUB, tile))
        cash_sum = lax.dot_general(cash, picked, LANES, preferred_element_type=F32)
        for i in range(span):
            acc[moment_at + i : moment_at + i + 1, :] += cash_sum[
                0:1, i * BLOCK : (i + 1) * BLOCK
            ]
        return carry

    lax.fori_loop(0, share_tiles, basis_tile, 0)
    advance(1, 0)

    half_rows = acc.shape[0] // 2
    piece_rows = acc.shape[0] // n_p
    partner = (p + 1 - 2 * core, s)

    def half_at(c):
        return pl.ds(pl.multiple_of(c * half_rows, SUB), half_rows)

    def piece_at(c, zz):
        return pl.ds(pl.multiple_of(c * half_rows + zz * piece_rows, SUB), piece_rows)

    def z_peer(d):
        other = lax.rem(z + d, n_z)
        return other, (2 * other + core, s)

    def level_rows(count):
        def rows_of(c, zz):
            at = c * half_rows + zz * piece_rows + lax.broadcasted_iota(
                jnp.int32, (piece_rows, BLOCK), 0
            )
            return jnp.where(at < moment_at, LEVELS / count, LEVELS / (4.0 * count))

        return rows_of

    core_copy = remote(
        acc.at[half_at(1 - core)], core_recv, c1_send.at[0], c1_recv.at[0], partner
    )
    core_copy.start()
    core_copy.wait_recv()
    chip_scale = level_rows(2 * share)
    for zz in range(n_z):
        both = acc[piece_at(core, zz), :] + core_recv[zz * piece_rows : (zz + 1) * piece_rows, :]
        acc[piece_at(core, zz), :] = both
        z_piece[zz] = levels(both * chip_scale(core, zz))
    z_copies = []
    for d in range(1, n_z):
        other, device = z_peer(d)
        z_copies.append(
            remote(z_piece.at[other], z_recv.at[d], z_send.at[d], z_rcv.at[d], device)
        )
    for copy in z_copies:
        copy.start()
    advance(0, 2)
    for copy in z_copies:
        copy.wait_recv()
    mine = acc[piece_at(core, z), :]
    grain = 1.0 / level_rows(2 * share)(core, z)
    for d in range(1, n_z):
        mine = mine + widen(z_recv[d]) * grain
    piece[...] = mine
    x_piece[...] = levels(mine * level_rows(n_p * share)(core, z))
    x_copies = [
        remote(x_piece, x_recv.at[r], x_send.at[r], x_rcv.at[r], stock(r)) for r in range(1, n_s)
    ]
    for copy in x_copies:
        copy.start()
    advance(4, 2)
    for copy in x_copies:
        copy.wait_recv()
    mine = piece[...]
    grain = 1.0 / level_rows(n_p * share)(core, z)
    for r in range(1, n_s):
        mine = mine + widen(x_recv[r]) * grain
    total[piece_at(core, z), :] = mine

    def spread(slot, zz):
        return remote(
            total.at[piece_at(core, zz)], total.at[piece_at(core, zz)],
            c5_send.at[slot], c5_recv.at[slot], partner,
        )

    back_copies = []
    for d in range(1, n_z):
        _, device = z_peer(d)
        back_copies.append(
            remote(
                total.at[piece_at(core, z)], total.at[piece_at(core, z)],
                z4_send.at[d], z4_recv.at[d], device,
            )
        )
    for copy in back_copies:
        copy.start()
    core_copies = [spread(0, z)]
    core_copies[0].start()
    for d in range(1, n_z):
        back_copies[d - 1].wait_recv()
        copy = spread(d, lax.rem(z - d + n_z, n_z))
        copy.start()
        core_copies.append(copy)
    for copy in core_copies:
        copy.wait_recv()
    advance(1, 3)

    scale = 1.0 / path_count
    ridge = jnp.where(
        lax.broadcasted_iota(jnp.int32, (BLOCK, BLOCK), 0)
        == lax.broadcasted_iota(jnp.int32, (BLOCK, BLOCK), 1), ridge_weight, 0.0,
    )
    for at, (i, j) in enumerate(pairs):
        block = total[at * BLOCK : (at + 1) * BLOCK, :] * scale
        if i == j:
            system[i * BLOCK : (i + 1) * BLOCK, j * BLOCK : (j + 1) * BLOCK] = block + ridge
        else:
            system[i * BLOCK : (i + 1) * BLOCK, j * BLOCK : (j + 1) * BLOCK] = block
            system[j * BLOCK : (j + 1) * BLOCK, i * BLOCK : (i + 1) * BLOCK] = block.T
    moment[...] = jnp.zeros_like(moment)
    for i in range(span):
        moment[0:1, i * BLOCK : (i + 1) * BLOCK] = (
            total[moment_at + i : moment_at + i + 1, :] * scale
        )
    solve_sent, solve_passed = sent[0], passed[0]
    solve_steps = functions // BLOCK

    def during_solve(k):
        gather_send(solve_sent + k)
        gather_pass(solve_passed + k)

    solve(system, moment, inverse, reduced, tile_v, coef, during_solve)
    sent[0] += solve_steps
    passed[0] += solve_steps

    high, middle, low = pieces(coef[0:1, :])
    stack = jnp.concatenate([high, middle, low, jnp.zeros((5, functions), BF16)], axis=0)

    def value_tile(t, carry):
        here = columns(t)
        parts = jnp.dot(stack, basis_v[:, here], preferred_element_type=F32)
        value_v[s, :, here] = parts[0:1] + parts[1:2] + parts[2:3]
        return carry

    lax.fori_loop(0, share_tiles, value_tile, 0)
    value_copies = [
        remote(value_v.at[s], value_v.at[s], v_send.at[r], v_recv.at[r], stock(r))
        for r in range(1, n_s)
    ]
    for copy in value_copies:
        copy.start()
    advance(2, 2)
    own_copy.wait()
    shocks_copy.wait()
    for copy in value_copies:
        copy.wait_recv()
    advance(chunks, 0)
    first_left = passed[0]
    ahead = 4 + WIDE
    wide_tiles = share_tiles // WIDE

    def wide_columns(k):
        return pl.ds(pl.multiple_of(k * WIDE * tile, WIDE * tile), WIDE * tile)

    def delta_copy(k):
        return pltpu.make_async_copy(
            delta_v.at[:, wide_columns(k)], delta_ref.at[:, wide_columns(k)], delta_sem.at[k]
        )

    def adjoint_tile(k, carry):
        for c in range(WIDE):
            chunk = k * WIDE + c
            if square:
                ready = chunk + ahead

                @pl.when(jnp.logical_and(ready >= first_left, ready < chunks))
                def _():
                    gather_pass(ready)

        for c in range(WIDE):
            chunk = k * WIDE + c
            if square:
                passed_chunk(2, 1, 2, chunk).wait_recv()
                passed_chunk(3, 2, 1, chunk).wait_recv()
            else:
                for r in range(1, n_s):
                    own_chunk(r - 1, r, chunk).wait_recv()
        width = WIDE * tile
        here = pl.ds(pl.multiple_of(k * width, width), width)
        gathered = whole[:, :, here].reshape(n_s * rows, width)
        value = value_v[
            k // wide_tiles, :, pl.ds(pl.multiple_of(lax.rem(k, wide_tiles) * width, width), width)
        ]
        mixed = jnp.dot(split_v[...], gathered, preferred_element_type=F32)
        linear = whole[s, :, here].astype(F32)
        gains = [exercise_ref[d : d + 1, here].astype(F32) * value for d in range(STEPS)]
        strikes = lax.broadcasted_iota(jnp.int32, (BLOCK, width), 0).astype(jnp.int16)
        deposit = jnp.zeros(surface_acc.shape, F32)
        for date in range(STEPS - 1, -1, -1):
            at = (STEPS - 1 - date) * rows
            linear = linear + mixed[0:rows]
            adjoint = linear if at == 0 else linear + mixed[at : at + rows]
            for later in range(date, STEPS):
                lift = jnp.concatenate([basket_v[later - date]] * (width // BLOCK), axis=1)
                adjoint = adjoint + lift * gains[later]
            if date == 0:
                delta_v[:, here] = adjoint
            vega = (adjoint * shocks_v[date, :, here].astype(F32)).astype(BF16)
            bucket = bucket_ref[date : date + 1, here]
            spot = (bucket % BLOCK).astype(jnp.int16)
            group = (bucket // BLOCK).astype(jnp.int16)
            one_hot = jnp.where(spot == strikes, BF16(1), BF16(0))
            grouped = jnp.concatenate(
                [jnp.where(group == g, vega, BF16(0)) for g in range(NK // BLOCK)], axis=0
            )
            deposit = deposit + lax.dot_general(
                one_hot, grouped, LANES, preferred_element_type=F32
            )
        surface_acc[...] += deposit
        delta_copy(k).start()
        return carry

    for k in range(first_left, min(ahead, chunks)):
        gather_pass(k)
    lax.fori_loop(0, chunks // WIDE, adjoint_tile, 0)

    own_strikes = NK // n_p
    surface_recv[0] = jnp.concatenate(
        [surface_acc[:, g * rows : (g + 1) * rows] for g in range(NK // BLOCK)], axis=0
    ).reshape(n_p, own_strikes, rows)
    surface_copies = []
    for d in range(1, n_p):
        other = lax.rem(p + d, n_p)
        surface_copies.append(
            remote(
                surface_recv.at[0, other], surface_recv.at[1, d], s_send.at[d], s_recv.at[d],
                (other, s),
            )
        )
    for copy in surface_copies:
        copy.start()
    for copy in surface_copies:
        copy.wait_recv()
    own = surface_recv[0, p]
    for d in range(1, n_p):
        own = own + surface_recv[1, d]
    surface_ref[...] = own

    for copy in surface_copies + value_copies + x_copies + z_copies + back_copies + core_copies:
        copy.wait_send()
    core_copy.wait_send()
    for copies in factor_sends:
        for copy in copies:
            copy.wait_send()

    def drain(k, carry):
        for copy in chunk_copies(k):
            copy.wait_send()
        return carry

    lax.fori_loop(0, chunks, drain, 0)
    for k in range(chunks // WIDE):
        delta_copy(k).wait()


def per_device(
    n_p, n_s, prices, loadings, basis_w, basis_bias, payoff, in_fit, cotangent, shocks, corr_gen,
    basket, exercise, bucket,
):
    rows, paths = prices.shape
    rank, functions = basis_w.shape
    share = paths // n_s
    tile = min(TILE, share)
    chunks = paths // tile
    total_rows = sum_rows(functions, n_p)
    n_z = n_p // 2
    kinds = 4 if n_s == 4 else n_s - 1
    slots = 6 if n_s == 4 else 2 * (n_s - 1)
    vmem = pl.BlockSpec(memory_space=pltpu.VMEM)
    hbm = pl.BlockSpec(memory_space=pl.ANY)
    dma = pltpu.SemaphoreType.DMA
    delta, surface = pl.pallas_call(
        functools.partial(step_kernel, n_p, n_s, float(paths * n_p)),
        in_specs=[hbm] * 12,
        out_specs=[hbm, vmem],
        out_shape=[
            jax.ShapeDtypeStruct((rows, paths), F32),
            jax.ShapeDtypeStruct((NK // n_p, rows), F32),
        ],
        scratch_shapes=[
            pltpu.VMEM((rank, rows), BF16),
            pltpu.VMEM((rank, functions), F32),
            pltpu.VMEM((1, functions), F32),
            pltpu.VMEM((paths // BLOCK, BLOCK), BF16),
            pltpu.VMEM((1, paths), jnp.int32),
            pltpu.VMEM((n_s * rows, n_s * rows), BF16),
            pltpu.VMEM((1, n_s * rows), F32),
            pltpu.VMEM((STEPS, paths), jnp.int32),
            pltpu.VMEM((STEPS, paths), jnp.int32),
            pltpu.VMEM((rows, paths), BF16),
            pltpu.VMEM((n_s, rows, paths), BF16),
            pltpu.VMEM((STEPS, rows, paths), BF16),
            pltpu.VMEM((rows, paths), F32),
            pltpu.VMEM((n_s, rank, share), F32),
            pltpu.VMEM((slots, rank, share // 2), I16),
            pltpu.VMEM((slots, rank, share // 2), I16),
            pltpu.VMEM((slots, rank, BLOCK), F32),
            pltpu.VMEM((slots, rank, BLOCK), F32),
            pltpu.VMEM((functions, 6 * rank + PACK), BF16),
            pltpu.VMEM((functions, share), BF16),
            pltpu.VMEM((total_rows, BLOCK), F32),
            pltpu.VMEM((total_rows // 2, BLOCK), F32),
            pltpu.VMEM((n_z, total_rows // n_p, BLOCK), I16),
            pltpu.VMEM((n_z, total_rows // n_p, BLOCK), I16),
            pltpu.VMEM((total_rows // n_p, BLOCK), F32),
            pltpu.VMEM((total_rows // n_p, BLOCK), I16),
            pltpu.VMEM((n_s, total_rows // n_p, BLOCK), I16),
            pltpu.VMEM((total_rows, BLOCK), F32),
            pltpu.VMEM((functions, functions), F32),
            pltpu.VMEM((SUB, functions), F32),
            pltpu.VMEM((functions, BLOCK), F32),
            pltpu.VMEM((functions, functions), F32),
            pltpu.VMEM((BLOCK, BLOCK), F32),
            pltpu.VMEM((SUB, functions), F32),
            pltpu.VMEM((n_s, 1, share), F32),
            pltpu.VMEM((STEPS * rows, n_s * rows), BF16),
            pltpu.VMEM((STEPS, rows, BLOCK), F32),
            pltpu.VMEM((BLOCK, NK // BLOCK * rows), F32),
            pltpu.VMEM((2, n_p, NK // n_p, rows), F32),
            dma((12,)), dma((chunks,)), dma((slots,)), dma((slots,)), dma((slots,)), dma((slots,)),
            dma((kinds, chunks)),
            dma((kinds, chunks)), dma((1,)), dma((1,)), dma((n_z,)), dma((n_z,)), dma((n_s,)),
            dma((n_s,)), dma((n_z,)), dma((n_z,)), dma((n_z,)), dma((n_z,)), dma((n_s,)),
            dma((n_s,)), dma((n_p,)), dma((n_p,)),
        ],
        compiler_params=pltpu.CompilerParams(
            collective_id=0, has_side_effects=True, vmem_limit_bytes=62 * 1024 * 1024
        ),
        name="bermudan_step",
    )(
        prices, loadings.T, basis_w, basis_bias[None, :], payoff.reshape(-1, BLOCK), in_fit[None, :], cotangent,
        shocks, corr_gen, basket[None, :], exercise, bucket,
    )
    return delta, surface.T


def solution(mesh):
    n_p, n_s = mesh.shape["paths"], mesh.shape["stocks"]
    return jax.shard_map(
        functools.partial(per_device, n_p, n_s),
        mesh=mesh,
        in_specs=(
            P("stocks", "paths"),
            P("stocks", None),
            P(),
            P(),
            P("paths"),
            P("paths"),
            P("stocks", "paths"),
            P(None, "stocks", "paths"),
            P(),
            P(),
            P(None, "paths"),
            P(None, "paths"),
        ),
        out_specs=(P("stocks", "paths"), P("stocks", "paths")),
        check_vma=False,
    )
```
